8 devices in a mesh: rep: 1 (over z), dp: 8 (over x, y, core).
Axes of the slice: x: 2, y: 2, z: 1, core: 2. Of those that a mesh axis runs over, the one named last changes fastest.
Arguments:
- x: bfloat16 [8, 2048, 1024], P(('rep', 'dp'))
- dy: bfloat16 [8, 2048, 1024], P(('rep', 'dp'))
- w_gate: bfloat16 [2, 1024, 3328], replicated
- w_up: bfloat16 [2, 1024, 3328], replicated
- w_down: bfloat16 [2, 3328, 1024], replicated
- m_w_gate: float32 [2, 1024, 3328], replicated
- m_w_up: float32 [2, 1024, 3328], replicated
- m_w_down: float32 [2, 3328, 1024], replicated
- v_w_gate: float32 [2, 1024, 3328], replicated
- v_w_up: float32 [2, 1024, 3328], replicated
- v_w_down: float32 [2, 3328, 1024], replicated
Outputs:
- output 1: bfloat16 [2, 1024, 3328], P('rep')
- output 2: bfloat16 [2, 1024, 3328], P('rep')
- output 3: bfloat16 [2, 3328, 1024], P('rep')
- output 4: float32 [2, 1024, 3328], P('rep')
- output 5: float32 [2, 1024, 3328], P('rep')
- output 6: float32 [2, 3328, 1024], P('rep')
- output 7: float32 [2, 1024, 3328], P('rep')
- output 8: float32 [2, 1024, 3328], P('rep')
- output 9: float32 [2, 3328, 1024], P('rep')
All inputs are finite; a program needn't handle non-finite values.
Results may differ from the reference program's by a relative error of at most 0.0229.
Values are sent between devices in bfloat16 or wider.
A program may use at most 2.75 GiB of HBM per device.

```python
import jax
import jax.numpy as jnp
from jax import lax

SEQUENCES = 8
TOKENS = 2048
D = 1024
FF = 3328
LAYERS = 2
NAMES = ("w_gate", "w_up", "w_down")
SHAPES = {"w_gate": (LAYERS, D, FF), "w_up": (LAYERS, D, FF), "w_down": (LAYERS, FF, D)}


def bump(key, n, height):
    away = (jnp.arange(n, dtype=jnp.int32) - jax.random.randint(key, (), 0, n, jnp.int32)) % n
    return jnp.where(away < n // 8, height, 1.0)


def together(key, own, strength):
    shared = jax.random.normal(key, own.shape[1:], jnp.float32)
    return (own + strength * shared) * lax.rsqrt(1 + strength * strength)


def setup_inputs(seed: int = 0, part: int = 0) -> dict:
    kx, kdy, ka, kb, kz, kf, kh, kl, *keys = jax.random.split(jax.random.key(seed), 8 + 3 * len(NAMES))
    kx, kdy, ka, kb = (jax.random.fold_in(k, part) for k in (kx, kdy, ka, kb))
    kw, km, kv = (keys[i::3] for i in range(3))
    shape = (SEQUENCES, TOKENS, D)
    much_x, much_dy = jax.random.uniform(kz, (2,), jnp.float32, 0.0, 1.0)
    loud = 2.0 ** jax.random.uniform(jax.random.fold_in(kz, 1), (), jnp.float32, -1.0, 2.0)
    layers = 2.0 ** jax.random.uniform(kl, (LAYERS, 1, 1), jnp.float32, -1.0, 1.0)
    x = together(ka, jax.random.normal(kx, shape, jnp.float32), much_x) * bump(kf, D, 4.0)
    dy = together(kb, jax.random.normal(kdy, shape, jnp.float32), much_dy)
    drawn = {"x": x.astype(jnp.bfloat16), "dy": (loud * dy * (SEQUENCES * TOKENS) ** -0.5).astype(jnp.bfloat16)}
    for key, name in zip(kw, NAMES, strict=True):
        w = jax.random.normal(key, SHAPES[name], jnp.float32) * SHAPES[name][1] ** -0.5
        drawn[name] = (w * {"w_gate": 1.0, "w_up": bump(kh, FF, 4.0), "w_down": layers}[name]).astype(jnp.bfloat16)
    for key, name in zip(km, NAMES, strict=True):
        drawn[f"m_{name}"] = 0.1 * jax.random.normal(key, SHAPES[name], jnp.float32)
    for key, name in zip(kv, NAMES, strict=True):
        drawn[f"v_{name}"] = jax.random.uniform(key, SHAPES[name], jnp.float32, 0.005, 0.015)
    return drawn


def matmul(a, w):
    return jnp.dot(a, w, preferred_element_type=jnp.float32).astype(jnp.bfloat16)


def normed(h):
    wide = h.astype(jnp.float32)
    scale = lax.rsqrt(jnp.mean(wide**2, -1, keepdims=True) + 1e-6)
    return (wide * scale).astype(jnp.bfloat16)


def layer(h, w):
    a = normed(h)
    gate = jnp.dot(a, w["w_gate"], preferred_element_type=jnp.float32)
    up = jnp.dot(a, w["w_up"], preferred_element_type=jnp.float32)
    return h + matmul((jax.nn.silu(gate) * up).astype(jnp.bfloat16), w["w_down"])


def adamw(w, m, v, g):
    m = 0.9 * m + 0.1 * g
    v = 0.95 * v + 0.05 * g * g
    step = m * lax.rsqrt(v + 1e-8) + 0.1 * w
    return (w - 0.02 * step).astype(jnp.bfloat16), m, v


def stack(weights, h):
    return lax.scan(lambda h, w: (layer(h, w), None), h, weights)[0]


def reference(x, dy, w_gate, w_up, w_down, m_w_gate, m_w_up, m_w_down, v_w_gate, v_w_up, v_w_down):
    weights = dict(zip(NAMES, (w_gate, w_up, w_down), strict=True))

    def take(so_far, sequence):
        h, by_y = sequence
        _, back = jax.vjp(lambda w: stack(w, h), weights)
        return jax.tree.map(lambda total, term: total + term.astype(jnp.float32), so_far, back(by_y)[0]), None

    none_yet = {name: jnp.zeros(w.shape, jnp.float32) for name, w in weights.items()}
    by_weights, _ = lax.scan(take, none_yet, (x, dy))
    gradients = [by_weights[name].astype(jnp.bfloat16).astype(jnp.float32) for name in NAMES]
    new = [
        adamw(w.astype(jnp.float32), m, v, g)
        for w, m, v, g in zip((w_gate, w_up, w_down), (m_w_gate, m_w_up, m_w_down), (v_w_gate, v_w_up, v_w_down), gradients, strict=True)
    ]
    return tuple(one[which] for which in range(3) for one in new)
```

```python
import functools

import jax
import jax.numpy as jnp
from jax import lax
from jax.experimental import pallas as pl
from jax.experimental.pallas import tpu as pltpu
from jax.sharding import PartitionSpec as P

F32, BF16 = jnp.float32, jnp.bfloat16
T, D, FF = 2048, 1024, 3328
BLK = 256
NB = FF // BLK
CH = 512
EPS = 1e-6
MESH = pl.DeviceIdType.MESH
VMEM_LIMIT = 64 * 1024 * 1024 - 65536 - 1024 * 1024


def dot(a, b):
    return lax.dot_general(a, b, (((1,), (0,)), ((), ())), preferred_element_type=F32)


def dot_nt(a, b):
    return lax.dot_general(a, b, (((1,), (1,)), ((), ())), preferred_element_type=F32)


def whole(shape):
    return pl.BlockSpec(shape, lambda *_: (0,) * len(shape), pipeline_mode=pl.Buffered(1))


def norm_rows(h):
    wide = h.astype(F32)
    scale = lax.rsqrt(jnp.mean(wide * wide, -1, keepdims=True) + EPS)
    return (wide * scale).astype(BF16)


def forward_kernel(x_ref, wg_ref, wu_ref, wd_ref, gate_ref, up_ref, h_ref, a_ref, a0, acc):
    j = pl.program_id(0)

    @pl.when(j == 0)
    def _():
        def prepare(i, _):
            rows = pl.ds(pl.multiple_of(i * CH, CH), CH)
            a0[rows, :] = norm_rows(x_ref[rows, :])
            acc[rows, :] = jnp.zeros((CH, D), F32)
            return 0

        lax.fori_loop(0, T // CH, prepare, 0)

    def chunk(i, _):
        rows = pl.ds(pl.multiple_of(i * CH, CH), CH)
        a = a0[rows, :]
        g = dot(a, wg_ref[0])
        u = dot(a, wu_ref[0])
        gate_ref[rows, :] = g
        up_ref[rows, :] = u
        hid = (g * jax.nn.sigmoid(g) * u).astype(BF16)
        acc[rows, :] += dot(hid, wd_ref[0])
        return 0

    lax.fori_loop(0, T // CH, chunk, 0)

    @pl.when(j == NB - 1)
    def _():
        def finish(i, _):
            rows = pl.ds(pl.multiple_of(i * CH, CH), CH)
            h = (x_ref[rows, :].astype(F32) + acc[rows, :].astype(BF16).astype(F32)).astype(BF16)
            h_ref[rows, :] = h
            a_ref[rows, :] = norm_rows(h)
            return 0

        lax.fori_loop(0, T // CH, finish, 0)


def forward(x, wg, wu, wd):
    return pl.pallas_call(
        forward_kernel,
        grid=(NB,),
        in_specs=[
            whole((T, D)),
            pl.BlockSpec((1, D, BLK), lambda j: (0, 0, j)),
            pl.BlockSpec((1, D, BLK), lambda j: (0, 0, j)),
            pl.BlockSpec((1, BLK, D), lambda j: (0, j, 0)),
        ],
        out_specs=[
            pl.BlockSpec((T, BLK), lambda j: (0, j)),
            pl.BlockSpec((T, BLK), lambda j: (0, j)),
            whole((T, D)),
            whole((T, D)),
        ],
        out_shape=[
            jax.ShapeDtypeStruct((T, FF), F32),
            jax.ShapeDtypeStruct((T, FF), F32),
            jax.ShapeDtypeStruct((T, D), BF16),
            jax.ShapeDtypeStruct((T, D), BF16),
        ],
        scratch_shapes=[pltpu.VMEM((T, D), BF16), pltpu.VMEM((T, D), F32)],
        compiler_params=pltpu.CompilerParams(vmem_limit_bytes=VMEM_LIMIT),
        cost_estimate=pl.CostEstimate(flops=6 * T * D * FF, bytes_accessed=8 * T * FF, transcendentals=T * FF),
        name="fwd0",
    )(x, wg, wu, wd)


SLOTS = 3


def store_pieces(g_buf, q, value):
    value = value.astype(BF16)
    for c in range(2):
        for ab in range(2):
            for s1 in range(2):
                for s2 in range(2):
                    x, y = (s1, s2) if ab == 0 else (s2, s1)
                    d = x * 4 + y * 2 + c
                    if q < 2:
                        r = d * 128 + ab * 64
                        g_buf[c, ab, s1, s2, q] = value[r : r + 64]
                    else:
                        r = d * 32 + ab * 16
                        for k in range(4):
                            g_buf[c, ab, s1, s2, q, k * 16 : k * 16 + 16] = value[r : r + 16, k * 256 : k * 256 + 256]


class Exchange:
    def __init__(self, bufs, sems):
        self.g, self.h, self.q, self.r0, self.r1, self.r2 = bufs
        self.send, self.recv, self.ahead = sems
        me = lax.axis_index("dp")
        self.rep = lax.axis_index("rep")
        self.x, self.y, self.c = me // 4, (me // 2) % 2, me % 2
        self.nx = (1 - self.x) * 4 + self.y * 2 + self.c
        self.ny = self.x * 4 + (1 - self.y) * 2 + self.c
        self.nc = self.x * 4 + self.y * 2 + (1 - self.c)

    def copy(self, kind, block, src, dst, to):
        slot = lax.rem(block, SLOTS)
        return pltpu.make_async_remote_copy(
            src_ref=src,
            dst_ref=dst,
            send_sem=self.send.at[kind, slot],
            recv_sem=self.recv.at[kind, slot],
            device_id=(self.rep, to),
            device_id_type=MESH,
        )

    def pair(self, b):
        return [self.copy(0, b, self.g.at[1 - self.c], self.r0.at[lax.rem(b, SLOTS)], self.nc)]

    def first(self, b):
        s = lax.rem(b, SLOTS)
        return [
            self.copy(1, b, self.h.at[0, 1 - self.x], self.r1.at[s, 0], self.nx),
            self.copy(2, b, self.h.at[1, 1 - self.y], self.r1.at[s, 1], self.ny),
        ]

    def second(self, b):
        s = lax.rem(b, SLOTS)
        return [
            self.copy(3, b, self.q.at[0, 1 - self.y], self.r2.at[s, 0], self.ny),
            self.copy(4, b, self.q.at[1, 1 - self.x], self.r2.at[s, 1], self.nx),
        ]

    def greet(self):
        barrier = pltpu.get_barrier_semaphore()
        for n in (self.nx, self.ny, self.nc):
            pl.semaphore_signal(barrier, inc=1, device_id=(self.rep, n), device_id_type=MESH)
        pl.semaphore_wait(barrier, 3)

    def wait_peers(self, count=1):
        for k in range(3):
            pl.semaphore_wait(self.ahead.at[k], count)

    def tell_peers(self):
        for k, n in enumerate((self.nx, self.ny, self.nc)):
            pl.semaphore_signal(self.ahead.at[k], inc=1, device_id=(self.rep, n), device_id_type=MESH)

    def stages(self, t, e_ref):
        @pl.when(t >= 3)
        def _():
            b = t - 3
            s = lax.rem(b, SLOTS)
            for cp in self.second(b):
                cp.wait()
            for ab, s2 in ((0, self.y), (1, self.x)):
                e_ref[0, ab] = (self.q[ab, s2].astype(F32) + self.r2[s, ab].astype(F32)).astype(BF16)

        @pl.when((t >= 2) & (t < NB + 2))
        def _():
            b = t - 2
            s = lax.rem(b, SLOTS)
            for cp in self.first(b):
                cp.wait()
            for ab, s1 in ((0, self.x), (1, self.y)):
                for s2 in range(2):
                    self.q[ab, s2] = (self.h[ab, s1, s2].astype(F32) + self.r1[s, ab, s2].astype(F32)).astype(BF16)
            for cp in self.second(b):
                cp.start()

        @pl.when((t >= 1) & (t < NB + 1))
        def _():
            b = t - 1
            s = lax.rem(b, SLOTS)
            for cp in self.pair(b):
                cp.wait()

            def add(k, _):
                ab, s1, s2 = k // 4, (k // 2) % 2, k % 2
                self.h[ab, s1, s2] = (self.g[self.c, ab, s1, s2].astype(F32) + self.r0[s, ab, s1, s2].astype(F32)).astype(BF16)
                return 0

            lax.fori_loop(0, 8, add, 0)
            for cp in self.first(b):
                cp.start()


EXCHANGE_SCRATCH = [
    pltpu.VMEM((2, 2, 2, 2, 3, 64, BLK), BF16),
    pltpu.VMEM((2, 2, 2, 3, 64, BLK), BF16),
    pltpu.VMEM((2, 2, 3, 64, BLK), BF16),
    pltpu.VMEM((SLOTS, 2, 2, 2, 3, 64, BLK), BF16),
    pltpu.VMEM((SLOTS, 2, 2, 3, 64, BLK), BF16),
    pltpu.VMEM((SLOTS, 2, 3, 64, BLK), BF16),
    pltpu.SemaphoreType.DMA((5, SLOTS)),
    pltpu.SemaphoreType.DMA((5, SLOTS)),
    pltpu.SemaphoreType.REGULAR((3,)),
]
STEPS = NB + 3


def gate_grads(g, u, dh):
    s = jax.nn.sigmoid(g)
    sg = g * s
    hid = (sg * u).astype(BF16)
    dh = dh.astype(BF16).astype(F32)
    dgate = (dh * u * (s * (1.0 + g * (1.0 - s)))).astype(BF16)
    dup = (dh * sg).astype(BF16)
    return hid, dgate, dup


def weight_grads(ex, at_ref, dt_ref, hid_s, dg_s, du_s):
    store_pieces(ex.g, 0, dot(at_ref[...], dg_s[...]))
    store_pieces(ex.g, 1, dot(at_ref[...], du_s[...]))
    store_pieces(ex.g, 2, dot(dt_ref[...], hid_s[...]).T)


def around(ex, e_ref, compute):
    t = pl.program_id(0)

    @pl.when(t == 0)
    def _():
        ex.greet()

    @pl.when(t >= 2)
    def _():
        ex.wait_peers()

    ex.stages(t, e_ref)

    @pl.when(t < NB)
    def _():
        compute(t)
        for cp in ex.pair(t):
            cp.start()

    ex.tell_peers()

    @pl.when(t == STEPS - 1)
    def _():
        ex.wait_peers(2)


def last_layer_kernel(a_ref, at_ref, dy_ref, dyt_ref, h_ref, wg_ref, wu_ref, wd_ref, e_ref, dh_ref, acc, hid_s, dg_s, du_s, *scratch):
    ex = Exchange(scratch[:6], scratch[6:])

    def compute(t):
        @pl.when(t == 0)
        def _():
            acc[...] = jnp.zeros((T, D), F32)

        def chunk(i, _):
            rows = pl.ds(pl.multiple_of(i * CH, CH), CH)
            a = a_ref[rows, :]
            g = dot(a, wg_ref[0])
            u = dot(a, wu_ref[0])
            dh = dot_nt(dy_ref[rows, :], wd_ref[0])
            hid, dgate, dup = gate_grads(g, u, dh)
            hid_s[rows, :] = hid
            dg_s[rows, :] = dgate
            du_s[rows, :] = dup
            acc[rows, :] += dot_nt(dgate, wg_ref[0]) + dot_nt(dup, wu_ref[0])
            return 0

        lax.fori_loop(0, T // CH, chunk, 0)
        weight_grads(ex, at_ref, dyt_ref, hid_s, dg_s, du_s)

    around(ex, e_ref, compute)

    @pl.when(pl.program_id(0) == NB)
    def _():
        def chunk(i, _):
            rows = pl.ds(pl.multiple_of(i * CH, CH), CH)
            wide = h_ref[rows, :].astype(F32)
            da = acc[rows, :].astype(BF16).astype(F32)
            scale = lax.rsqrt(jnp.mean(wide * wide, -1, keepdims=True) + EPS)
            inner = jnp.mean(da * wide, -1, keepdims=True)
            back = (da * scale - wide * (scale * scale * scale * inner)).astype(BF16)
            dh_ref[rows, :] = (dy_ref[rows, :].astype(F32) + back.astype(F32)).astype(BF16)
            return 0

        lax.fori_loop(0, T // CH, chunk, 0)


def first_layer_kernel(at_ref, dh_ref, dht_ref, gate_ref, up_ref, wd_ref, e_ref, hid_s, dg_s, du_s, *scratch):
    ex = Exchange(scratch[:6], scratch[6:])

    def compute(t):
        def chunk(i, _):
            rows = pl.ds(pl.multiple_of(i * CH, CH), CH)
            dh = dot_nt(dh_ref[rows, :], wd_ref[0])
            hid, dgate, dup = gate_grads(gate_ref[rows, :], up_ref[rows, :], dh)
            hid_s[rows, :] = hid
            dg_s[rows, :] = dgate
            du_s[rows, :] = dup
            return 0

        lax.fori_loop(0, T // CH, chunk, 0)
        weight_grads(ex, at_ref, dht_ref, hid_s, dg_s, du_s)

    around(ex, e_ref, compute)


def at_step(t):
    return jnp.minimum(t, NB - 1)


PIECES = (2, 3, 64, BLK)
E_SPEC = pl.BlockSpec((1,) + PIECES, lambda t: (jnp.maximum(t - 3, 0), 0, 0, 0, 0))
E_SHAPE = jax.ShapeDtypeStruct((NB,) + PIECES, BF16)
HALVES = [pltpu.VMEM((T, BLK), BF16)] * 3


def last_layer(a, at, dy, dyt, h, wg, wu, wd):
    return pl.pallas_call(
        last_layer_kernel,
        grid=(STEPS,),
        in_specs=[
            whole((T, D)),
            whole((D, T)),
            whole((T, D)),
            whole((D, T)),
            whole((T, D)),
            pl.BlockSpec((1, D, BLK), lambda t: (1, 0, at_step(t))),
            pl.BlockSpec((1, D, BLK), lambda t: (1, 0, at_step(t))),
            pl.BlockSpec((1, BLK, D), lambda t: (1, at_step(t), 0)),
        ],
        out_specs=[E_SPEC, whole((T, D))],
        out_shape=[E_SHAPE, jax.ShapeDtypeStruct((T, D), BF16)],
        scratch_shapes=[pltpu.VMEM((T, D), F32), *HALVES, *EXCHANGE_SCRATCH],
        compiler_params=pltpu.CompilerParams(vmem_limit_bytes=VMEM_LIMIT, collective_id=0, has_side_effects=True),
        cost_estimate=pl.CostEstimate(flops=16 * T * D * FF, bytes_accessed=6 * D * FF, transcendentals=T * FF),
        name="last_layer",
    )(a, at, dy, dyt, h, wg, wu, wd)


def first_layer(at, dh, dht, gate, up, wd):
    return pl.pallas_call(
        first_layer_kernel,
        grid=(STEPS,),
        in_specs=[
            whole((D, T)),
            whole((T, D)),
            whole((D, T)),
            pl.BlockSpec((T, BLK), lambda t: (0, at_step(t))),
            pl.BlockSpec((T, BLK), lambda t: (0, at_step(t))),
            pl.BlockSpec((1, BLK, D), lambda t: (0, at_step(t), 0)),
        ],
        out_specs=[E_SPEC],
        out_shape=[E_SHAPE],
        scratch_shapes=[*HALVES, *EXCHANGE_SCRATCH],
        compiler_params=pltpu.CompilerParams(vmem_limit_bytes=VMEM_LIMIT, collective_id=1, has_side_effects=True),
        cost_estimate=pl.CostEstimate(flops=8 * T * D * FF, bytes_accessed=8 * T * FF, transcendentals=T * FF),
        name="first_layer",
    )(at, dh, dht, gate, up, wd)[0]


def adamw(w, m, v, g):
    m = 0.9 * m + 0.1 * g
    v = 0.95 * v + 0.05 * g * g
    step = m * lax.rsqrt(v + 1e-8) + 0.1 * w
    return (w - 0.02 * step).astype(BF16), m, v


def adamw_kernel(g_ref, *refs):
    ins, outs = refs[:9], refs[-9:]
    for q in range(3):
        w_ref, m_ref, v_ref = ins[q], ins[3 + q], ins[6 + q]
        wo_ref, mo_ref, vo_ref = outs[q], outs[3 + q], outs[6 + q]
        if q < 2:
            for d in range(8):
                for ab in range(2):
                    r = pl.ds(d * 128 + ab * 64, 64)
                    g = g_ref[d, 0, ab, q].astype(F32)
                    wo_ref[0, r, :], mo_ref[0, r, :], vo_ref[0, r, :] = adamw(w_ref[0, r, :].astype(F32), m_ref[0, r, :], v_ref[0, r, :], g)
        else:
            for d in range(8):
                for ab in range(2):
                    r = pl.ds(d * 32 + ab * 16, 16)
                    for k in range(4):
                        c = pl.ds(k * 256, 256)
                        g = g_ref[d, 0, ab, q, k * 16 : k * 16 + 16].astype(F32)
                        wo_ref[0, r, c], mo_ref[0, r, c], vo_ref[0, r, c] = adamw(
                            w_ref[0, r, c].astype(F32), m_ref[0, r, c], v_ref[0, r, c], g
                        )


def update(layer, g, arrays, before):
    wide = pl.BlockSpec((1, D, BLK), lambda j: (layer, 0, j))
    tall = pl.BlockSpec((1, BLK, D), lambda j: (layer, j, 0))
    specs = [wide, wide, tall] * 3
    shapes = [jax.ShapeDtypeStruct(a.shape, a.dtype) for a in arrays]
    held = [] if before is None else list(before)
    return pl.pallas_call(
        adamw_kernel,
        grid=(NB,),
        in_specs=[pl.BlockSpec((8, 1) + PIECES, lambda j: (0, j, 0, 0, 0, 0)), *specs, *[pl.BlockSpec(memory_space=pl.ANY)] * len(held)],
        out_specs=specs,
        out_shape=shapes,
        input_output_aliases={10 + i: i for i in range(len(held))},
        compiler_params=pltpu.CompilerParams(vmem_limit_bytes=VMEM_LIMIT),
        cost_estimate=pl.CostEstimate(flops=30 * 3 * D * FF, bytes_accessed=22 * 3 * D * FF, transcendentals=3 * D * FF),
        name=f"adamw{layer}",
    )(g, *arrays, *held)


def solution(mesh):
    def step(x, dy, wg, wu, wd, *moments):
        x, dy = x[0], dy[0]
        gate, up, h1, a1 = forward(x, wg, wu, wd)
        e1, dh1 = last_layer(a1, a1.T, dy, dy.T, h1, wg, wu, wd)
        g1 = lax.all_gather(e1, "dp", axis=0, tiled=False)
        e0 = first_layer(norm_rows(x).T, dh1, dh1.T, gate, up, wd)
        g0 = lax.all_gather(e0, "dp", axis=0, tiled=False)
        arrays = (wg, wu, wd, *moments)
        g1, e0 = lax.optimization_barrier((g1, e0))
        new = update(1, g1, arrays, None)
        return tuple(update(0, g0, arrays, new))

    return jax.shard_map(
        step,
        mesh=mesh,
        in_specs=(P(("rep", "dp"), None, None),) * 2 + (P(None, None, None),) * 9,
        out_specs=(P("rep", None, None),) * 9,
        check_vma=False,
    )
```

```python
import functools
import itertools

import jax
import jax.numpy as jnp
from jax import lax
from jax.experimental import pallas as pl
from jax.experimental.pallas import tpu as pltpu
from jax.sharding import PartitionSpec as P

F32, BF16 = jnp.float32, jnp.bfloat16
T, D, FF = 2048, 1024, 3328
BLK = 256
NB = FF // BLK
CH = 512
TURN = 256
EPS = 1e-6
MESH = pl.DeviceIdType.MESH
VMEM_LIMIT = 64 * 1024 * 1024 - 65536 - 1024 * 1024


def dot(a, b):
    return lax.dot_general(a, b, (((1,), (0,)), ((), ())), preferred_element_type=F32)


def dot_nt(a, b):
    return lax.dot_general(a, b, (((1,), (1,)), ((), ())), preferred_element_type=F32)


def whole(shape):
    return pl.BlockSpec(shape, lambda *_: (0,) * len(shape), pipeline_mode=pl.Buffered(1))


def norm_rows(h):
    wide = h.astype(F32)
    scale = lax.rsqrt(jnp.mean(wide * wide, -1, keepdims=True) + EPS)
    return (wide * scale).astype(BF16)


def turn_step(j):
    return jnp.minimum(j, T // TURN - 1)


def pipelined(front, back):
    chunks = [pl.ds(i * CH, CH) for i in range(T // CH)]
    front(chunks[0])
    for i, rows in enumerate(chunks):
        if i + 1 < len(chunks):
            front(chunks[i + 1])
        back(rows)


def forward_kernel(x_ref, dy_ref, wg_ref, wu_ref, wd_ref, gate_ref, up_ref, h_ref, a_ref, at_ref, dyt_ref, a0, acc):
    j = pl.program_id(0)

    @pl.when(j == 0)
    def _():
        def prepare(i, _):
            rows = pl.ds(pl.multiple_of(i * CH, CH), CH)
            a0[rows, :] = norm_rows(x_ref[rows, :])
            acc[rows, :] = jnp.zeros((CH, D), F32)
            return 0

        lax.fori_loop(0, T // CH, prepare, 0)

    def front(rows):
        a = a0[rows, :]
        gate_ref[rows, :] = dot(a, wg_ref[0])
        up_ref[rows, :] = dot(a, wu_ref[0])

    def back(rows):
        g = gate_ref[rows, :]
        hid = (g * jax.nn.sigmoid(g) * up_ref[rows, :]).astype(BF16)
        acc[rows, :] += dot(hid, wd_ref[0])

    at_ref[...] = a0[pl.ds(pl.multiple_of(turn_step(j) * TURN, TURN), TURN), :].T
    dyt_ref[...] = dy_ref[...].T
    pipelined(front, back)

    @pl.when(j == NB - 1)
    def _():
        def finish(i, _):
            rows = pl.ds(pl.multiple_of(i * CH, CH), CH)
            h = (x_ref[rows, :].astype(F32) + acc[rows, :].astype(BF16).astype(F32)).astype(BF16)
            h_ref[rows, :] = h
            a_ref[rows, :] = norm_rows(h)
            return 0

        lax.fori_loop(0, T // CH, finish, 0)


def forward(x, dy, wg, wu, wd):
    return pl.pallas_call(
        forward_kernel,
        grid=(NB,),
        in_specs=[
            whole((T, D)),
            pl.BlockSpec((TURN, D), lambda j: (turn_step(j), 0)),
            pl.BlockSpec((1, D, BLK), lambda j: (0, 0, j)),
            pl.BlockSpec((1, D, BLK), lambda j: (0, 0, j)),
            pl.BlockSpec((1, BLK, D), lambda j: (0, j, 0)),
        ],
        out_specs=[
            pl.BlockSpec((T, BLK), lambda j: (0, j)),
            pl.BlockSpec((T, BLK), lambda j: (0, j)),
            whole((T, D)),
            whole((T, D)),
            pl.BlockSpec((D, TURN), lambda j: (0, turn_step(j))),
            pl.BlockSpec((D, TURN), lambda j: (0, turn_step(j))),
        ],
        out_shape=[
            jax.ShapeDtypeStruct((T, FF), F32),
            jax.ShapeDtypeStruct((T, FF), F32),
            jax.ShapeDtypeStruct((T, D), BF16),
            jax.ShapeDtypeStruct((T, D), BF16),
            jax.ShapeDtypeStruct((D, T), BF16),
            jax.ShapeDtypeStruct((D, T), BF16),
        ],
        scratch_shapes=[pltpu.VMEM((T, D), BF16), pltpu.VMEM((T, D), F32)],
        compiler_params=pltpu.CompilerParams(vmem_limit_bytes=VMEM_LIMIT),
        cost_estimate=pl.CostEstimate(flops=6 * T * D * FF, bytes_accessed=8 * T * FF, transcendentals=T * FF),
        name="fwd0",
    )(x, dy, wg, wu, wd)


SLOTS = 3


def store_pieces(g_buf, slot, q, value):
    value = value.astype(BF16)
    for c in range(2):
        for ab in range(2):
            for s1 in range(2):
                for s2 in range(2):
                    x, y = (s1, s2) if ab == 0 else (s2, s1)
                    d = x * 4 + y * 2 + c
                    if q < 2:
                        r = d * 128 + ab * 64
                        g_buf[slot, c, ab, s1, s2, q] = value[r : r + 64]
                    else:
                        r = d * 32 + ab * 16
                        for k in range(4):
                            g_buf[slot, c, ab, s1, s2, q, k * 16 : k * 16 + 16] = value[r : r + 16, k * 256 : k * 256 + 256]


class Exchange:
    def __init__(self, scratch, f=None):
        self.g, self.h, self.q, self.e, self.r0, self.r1, self.r2 = scratch[:7]
        self.send, self.recv, self.keep, self.ahead = scratch[7:]
        self.f = f
        me = lax.axis_index("dp")
        self.rep = lax.axis_index("rep")
        self.x, self.y, self.c = me // 4, (me // 2) % 2, me % 2
        self.nx = (1 - self.x) * 4 + self.y * 2 + self.c
        self.ny = self.x * 4 + (1 - self.y) * 2 + self.c
        self.nc = self.x * 4 + self.y * 2 + (1 - self.c)

    def copy(self, kind, block, src, dst, to):
        slot = lax.rem(block, SLOTS)
        return pltpu.make_async_remote_copy(
            src_ref=src,
            dst_ref=dst,
            send_sem=self.send.at[kind, slot],
            recv_sem=self.recv.at[kind, slot],
            device_id=(self.rep, to),
            device_id_type=MESH,
        )

    def pair(self, b):
        return [self.copy(0, b, self.g.at[lax.rem(b, 2), 1 - self.c], self.r0.at[lax.rem(b, SLOTS)], self.nc)]

    def first(self, b):
        s = lax.rem(b, SLOTS)
        return [
            self.copy(1, b, self.h.at[0, 1 - self.x], self.r1.at[s, 0], self.nx),
            self.copy(2, b, self.h.at[1, 1 - self.y], self.r1.at[s, 1], self.ny),
        ]

    def second(self, b):
        s = lax.rem(b, SLOTS)
        return [
            self.copy(3, b, self.q.at[0, 1 - self.y], self.r2.at[s, 0], self.ny),
            self.copy(4, b, self.q.at[1, 1 - self.x], self.r2.at[s, 1], self.nx),
        ]

    def greet(self):
        barrier = pltpu.get_barrier_semaphore()
        for n in (self.nx, self.ny, self.nc):
            pl.semaphore_signal(barrier, inc=1, device_id=(self.rep, n), device_id_type=MESH)
        pl.semaphore_wait(barrier, 3)

    def wait_peers(self, count=1):
        for k in range(3):
            pl.semaphore_wait(self.ahead.at[k], count)

    def tell_peers(self):
        for k, n in enumerate((self.nx, self.ny, self.nc)):
            pl.semaphore_signal(self.ahead.at[k], inc=1, device_id=(self.rep, n), device_id_type=MESH)

    def mine(self, ab):
        return (self.x, self.y) if ab == 0 else (self.y, self.x)

    def own(self, b):
        return [pltpu.make_async_copy(self.e.at[ab], self.f.at[(b, self.c, ab, *self.mine(ab))], self.keep.at[ab]) for ab in range(2)]

    def back_first(self, b):
        return [self.copy(5 + ab, b, self.e.at[ab], self.f.at[(b, self.c, ab, *self.mine(ab))], (self.ny, self.nx)[ab]) for ab in range(2)]

    def back_second(self, b):
        out = []
        for ab in range(2):
            part = self.f.at[b, self.c, ab, self.mine(ab)[0]]
            out.append(self.copy(7 + ab, b, part, part, (self.nx, self.ny)[ab]))
        return out

    def back_pair(self, b):
        return [self.copy(9, b, self.f.at[b, self.c], self.f.at[b, self.c], self.nc)]

    def sums(self, b, out):
        s = lax.rem(b, SLOTS)
        for ab in range(2):
            s2 = self.mine(ab)[1]
            out[ab] = (self.q[ab, s2].astype(F32) + self.r2[s, ab].astype(F32)).astype(BF16)

    def stages(self, t, gathered, e_refs):
        def at(lag, end, begin=0):
            return (t >= begin + lag) & (t < end + lag)

        if gathered:

            @pl.when(at(6, gathered))
            def _():
                for cp in self.back_pair(t - 6):
                    cp.wait()

            @pl.when(at(5, gathered))
            def _():
                for cp in self.back_second(t - 5):
                    cp.wait()
                for cp in self.back_pair(t - 5):
                    cp.start()

            @pl.when(at(4, gathered))
            def _():
                for cp in self.own(t - 4) + self.back_first(t - 4):
                    cp.wait()
                for cp in self.back_second(t - 4):
                    cp.start()

        @pl.when(at(3, NB))
        def _():
            for cp in self.second(t - 3):
                cp.wait()

        if gathered:

            @pl.when(at(3, gathered))
            def _():
                b = t - 3
                self.sums(b, self.e)
                for cp in self.own(b) + self.back_first(b):
                    cp.start()

        for begin, end, e_ref in e_refs:

            @pl.when(at(3, end, begin))
            def _(e_ref=e_ref):
                self.sums(t - 3, e_ref.at[0])

        @pl.when(at(2, NB))
        def _():
            b = t - 2
            s = lax.rem(b, SLOTS)
            for cp in self.first(b):
                cp.wait()
            for ab in range(2):
                s1 = self.mine(ab)[0]
                for s2 in range(2):
                    self.q[ab, s2] = (self.h[ab, s1, s2].astype(F32) + self.r1[s, ab, s2].astype(F32)).astype(BF16)
            for cp in self.second(b):
                cp.start()

        @pl.when(at(1, NB))
        def _():
            b = t - 1
            s = lax.rem(b, SLOTS)
            g = lax.rem(b, 2)
            for cp in self.pair(b):
                cp.wait()

            def add(k, _):
                ab, s1, s2 = k // 4, (k // 2) % 2, k % 2
                self.h[ab, s1, s2] = (self.g[g, self.c, ab, s1, s2].astype(F32) + self.r0[s, ab, s1, s2].astype(F32)).astype(BF16)
                return 0

            lax.fori_loop(0, 8, add, 0)
            for cp in self.first(b):
                cp.start()


EXCHANGE_SCRATCH = [
    pltpu.VMEM((2, 2, 2, 2, 2, 3, 64, BLK), BF16),
    pltpu.VMEM((2, 2, 2, 3, 64, BLK), BF16),
    pltpu.VMEM((2, 2, 3, 64, BLK), BF16),
    pltpu.VMEM((2, 3, 64, BLK), BF16),
    pltpu.VMEM((SLOTS, 2, 2, 2, 3, 64, BLK), BF16),
    pltpu.VMEM((SLOTS, 2, 2, 3, 64, BLK), BF16),
    pltpu.VMEM((SLOTS, 2, 3, 64, BLK), BF16),
    pltpu.SemaphoreType.DMA((10, SLOTS)),
    pltpu.SemaphoreType.DMA((10, SLOTS)),
    pltpu.SemaphoreType.DMA((2,)),
    pltpu.SemaphoreType.REGULAR((3,)),
]
STEPS = NB + 3
GATHERED = 10
HALF = 7


def gate_grads(g, u, dh):
    s = jax.nn.sigmoid(g)
    sg = g * s
    hid = (sg * u).astype(BF16)
    dh = dh.astype(BF16).astype(F32)
    dgate = (dh * u * (s * (1.0 + g * (1.0 - s)))).astype(BF16)
    dup = (dh * sg).astype(BF16)
    return hid, dgate, dup


def weight_grads(ex, t, at_ref, dt_ref, hid_s, dg_s, du_s):
    slot = lax.rem(t, 2)
    store_pieces(ex.g, slot, 0, dot(at_ref[...], dg_s[...]))
    store_pieces(ex.g, slot, 1, dot(at_ref[...], du_s[...]))
    store_pieces(ex.g, slot, 2, dot(dt_ref[...], hid_s[...]).T)


def around(ex, gathered, e_refs, compute):
    t = pl.program_id(0)

    @pl.when(t == 0)
    def _():
        ex.greet()

    @pl.when(t >= 2)
    def _():
        ex.wait_peers()

    @pl.when(t < NB)
    def _():
        compute(t)
        for cp in ex.pair(t):
            cp.start()

    ex.stages(t, gathered, e_refs)
    ex.tell_peers()

    @pl.when(t == STEPS - 1)
    def _():
        ex.wait_peers(2)


def last_layer_kernel(a_ref, at_ref, dy_ref, dyt_ref, h_ref, wg_ref, wu_ref, wd_ref, e_ref, f_ref, dh_ref, acc, g_s, u_s, dh_s, hid_s, dg_s, du_s, *scratch):
    ex = Exchange(scratch, f_ref)

    def compute(t):
        @pl.when(t == 0)
        def _():
            acc[...] = jnp.zeros((T, D), F32)

        def front(rows):
            a = a_ref[rows, :]
            g_s[rows, :] = dot(a, wg_ref[0])
            u_s[rows, :] = dot(a, wu_ref[0])
            dh_s[rows, :] = dot_nt(dy_ref[rows, :], wd_ref[0])

        def back(rows):
            hid, dgate, dup = gate_grads(g_s[rows, :], u_s[rows, :], dh_s[rows, :])
            hid_s[rows, :] = hid
            dg_s[rows, :] = dgate
            du_s[rows, :] = dup
            acc[rows, :] += dot_nt(dgate, wg_ref[0]) + dot_nt(dup, wu_ref[0])

        pipelined(front, back)
        weight_grads(ex, t, at_ref, dyt_ref, hid_s, dg_s, du_s)

    around(ex, GATHERED, [(GATHERED, NB, e_ref)], compute)

    @pl.when(pl.program_id(0) == NB)
    def _():
        def chunk(i, _):
            rows = pl.ds(pl.multiple_of(i * CH, CH), CH)
            wide = h_ref[rows, :].astype(F32)
            da = acc[rows, :].astype(BF16).astype(F32)
            scale = lax.rsqrt(jnp.mean(wide * wide, -1, keepdims=True) + EPS)
            inner = jnp.mean(da * wide, -1, keepdims=True)
            back = (da * scale - wide * (scale * scale * scale * inner)).astype(BF16)
            dh_ref[rows, :] = (dy_ref[rows, :].astype(F32) + back.astype(F32)).astype(BF16)
            return 0

        lax.fori_loop(0, T // CH, chunk, 0)


def first_layer_kernel(at_ref, dh_ref, dht_ref, gate_ref, up_ref, wd_ref, ea_ref, eb_ref, dh_s, hid_s, dg_s, du_s, *scratch):
    ex = Exchange(scratch)

    def compute(t):
        def front(rows):
            dh_s[rows, :] = dot_nt(dh_ref[rows, :], wd_ref[0])

        def back(rows):
            hid, dgate, dup = gate_grads(gate_ref[rows, :], up_ref[rows, :], dh_s[rows, :])
            hid_s[rows, :] = hid
            dg_s[rows, :] = dgate
            du_s[rows, :] = dup

        pipelined(front, back)
        weight_grads(ex, t, at_ref, dht_ref, hid_s, dg_s, du_s)

    around(ex, 0, [(0, HALF, ea_ref), (HALF, NB, eb_ref)], compute)


def at_step(t):
    return jnp.minimum(t, NB - 1)


PIECES = (2, 3, 64, BLK)
FULL = (2, 2, 2, 2, 3, 64, BLK)


def sums_spec(begin, end):
    return pl.BlockSpec((1,) + PIECES, lambda t: (jnp.clip(t - 3 - begin, 0, end - begin - 1), 0, 0, 0, 0))


def sums_shape(begin, end):
    return jax.ShapeDtypeStruct((end - begin,) + PIECES, BF16)


HALVES = [pltpu.VMEM((T, BLK), BF16)] * 3


def last_layer(a, at, dy, dyt, h, wg, wu, wd):
    return pl.pallas_call(
        last_layer_kernel,
        grid=(STEPS,),
        in_specs=[
            whole((T, D)),
            whole((D, T)),
            whole((T, D)),
            whole((D, T)),
            whole((T, D)),
            pl.BlockSpec((1, D, BLK), lambda t: (1, 0, at_step(t))),
            pl.BlockSpec((1, D, BLK), lambda t: (1, 0, at_step(t))),
            pl.BlockSpec((1, BLK, D), lambda t: (1, at_step(t), 0)),
        ],
        out_specs=[sums_spec(GATHERED, NB), pl.BlockSpec(memory_space=pl.ANY), whole((T, D))],
        out_shape=[sums_shape(GATHERED, NB), jax.ShapeDtypeStruct((GATHERED,) + FULL, BF16), jax.ShapeDtypeStruct((T, D), BF16)],
        scratch_shapes=[pltpu.VMEM((T, D), F32), *[pltpu.VMEM((T, BLK), F32)] * 3, *HALVES, *EXCHANGE_SCRATCH],
        compiler_params=pltpu.CompilerParams(vmem_limit_bytes=VMEM_LIMIT, collective_id=0, has_side_effects=True),
        cost_estimate=pl.CostEstimate(flops=16 * T * D * FF, bytes_accessed=6 * D * FF, transcendentals=T * FF),
        name="last_layer",
    )(a, at, dy, dyt, h, wg, wu, wd)


def first_layer(at, dh, dht, gate, up, wd):
    return pl.pallas_call(
        first_layer_kernel,
        grid=(STEPS,),
        in_specs=[
            whole((D, T)),
            whole((T, D)),
            whole((D, T)),
            pl.BlockSpec((T, BLK), lambda t: (0, at_step(t))),
            pl.BlockSpec((T, BLK), lambda t: (0, at_step(t))),
            pl.BlockSpec((1, BLK, D), lambda t: (0, at_step(t), 0)),
        ],
        out_specs=[sums_spec(0, HALF), sums_spec(HALF, NB)],
        out_shape=[sums_shape(0, HALF), sums_shape(HALF, NB)],
        scratch_shapes=[pltpu.VMEM((T, BLK), F32), *HALVES, *EXCHANGE_SCRATCH],
        compiler_params=pltpu.CompilerParams(vmem_limit_bytes=VMEM_LIMIT, collective_id=1, has_side_effects=True),
        cost_estimate=pl.CostEstimate(flops=8 * T * D * FF, bytes_accessed=8 * T * FF, transcendentals=T * FF),
        name="first_layer",
    )(at, dh, dht, gate, up, wd)


def adamw(w, m, v, g):
    m = 0.9 * m + 0.1 * g
    v = 0.95 * v + 0.05 * g * g
    step = m * lax.rsqrt(v + 1e-8) + 0.1 * w
    return (w - 0.02 * step).astype(BF16), m, v


def adamw_kernel(own, g_ref, *refs):
    ins, outs = refs[:9], refs[-9:]
    for x, y, c, ab in itertools.product(range(2), repeat=4):
        d = x * 4 + y * 2 + c
        at = (d, 0, ab) if not own else (0, c, ab, x, y) if ab == 0 else (0, c, ab, y, x)
        for q in range(3):
            w_ref, m_ref, v_ref = ins[q], ins[3 + q], ins[6 + q]
            wo_ref, mo_ref, vo_ref = outs[q], outs[3 + q], outs[6 + q]
            if q < 2:
                parts = [(pl.ds(d * 128 + ab * 64, 64), slice(None), slice(None))]
            else:
                parts = [(pl.ds(d * 32 + ab * 16, 16), pl.ds(k * 256, 256), pl.ds(k * 16, 16)) for k in range(4)]
            for r, cols, of in parts:
                g = g_ref[(*at, q, of)].astype(F32)
                wo_ref[0, r, cols], mo_ref[0, r, cols], vo_ref[0, r, cols] = adamw(
                    w_ref[0, r, cols].astype(F32), m_ref[0, r, cols], v_ref[0, r, cols], g
                )


def update(layer, begin, g, arrays, before):
    own = g.ndim == 8
    count = g.shape[0] if own else g.shape[1]
    g_spec = pl.BlockSpec((1,) + FULL, lambda j: (j,) + (0,) * 7) if own else pl.BlockSpec((8, 1) + PIECES, lambda j: (0, j, 0, 0, 0, 0))
    wide = pl.BlockSpec((1, D, BLK), lambda j: (layer, 0, begin + j))
    tall = pl.BlockSpec((1, BLK, D), lambda j: (layer, begin + j, 0))
    specs = [wide, wide, tall] * 3
    held = [] if before is None else list(before)
    size = 3 * D * BLK * count
    return pl.pallas_call(
        functools.partial(adamw_kernel, own),
        grid=(count,),
        in_specs=[g_spec, *specs, *[pl.BlockSpec(memory_space=pl.ANY)] * len(held)],
        out_specs=specs,
        out_shape=[jax.ShapeDtypeStruct(a.shape, a.dtype) for a in arrays],
        input_output_aliases={10 + i: i for i in range(len(held))},
        compiler_params=pltpu.CompilerParams(vmem_limit_bytes=VMEM_LIMIT),
        cost_estimate=pl.CostEstimate(flops=30 * size, bytes_accessed=22 * size, transcendentals=size),
        name=f"adamw{layer}_{begin}",
    )(g, *arrays, *held)


def solution(mesh):
    def step(x, dy, wg, wu, wd, *moments):
        x, dy = x[0], dy[0]
        gate, up, h1, a1, a0t, dyt = forward(x, dy, wg, wu, wd)
        e1, f1, dh1 = last_layer(a1, a1.T, dy, dyt, h1, wg, wu, wd)
        g1 = lax.all_gather(e1, "dp", axis=0, tiled=False)
        e0a, e0b = first_layer(a0t, dh1, dh1.T, gate, up, wd)
        g0a = lax.all_gather(e0a, "dp", axis=0, tiled=False)
        g0b = lax.all_gather(e0b, "dp", axis=0, tiled=False)
        f1, e0a = lax.optimization_barrier((f1, e0a))
        arrays = (wg, wu, wd, *moments)
        new = update(1, 0, f1, arrays, None)
        new = update(1, GATHERED, g1, arrays, new)
        new = update(0, 0, g0a, arrays, new)
        return tuple(update(0, HALF, g0b, arrays, new))

    return jax.shard_map(
        step,
        mesh=mesh,
        in_specs=(P(("rep", "dp"), None, None),) * 2 + (P(None, None, None),) * 9,
        out_specs=(P("rep", None, None),) * 9,
        check_vma=False,
    )
```

```python
import functools
import itertools

import jax
import jax.numpy as jnp
from jax import lax
from jax.experimental import pallas as pl
from jax.experimental.pallas import tpu as pltpu
from jax.sharding import PartitionSpec as P

F32, BF16 = jnp.float32, jnp.bfloat16
T, D, FF = 2048, 1024, 3328
BLK = 256
NB = FF // BLK
CH = 512
TURN = 256
EPS = 1e-6
MESH = pl.DeviceIdType.MESH
VMEM_LIMIT = 64 * 1024 * 1024 - 65536 - 1024 * 1024


def dot(a, b):
    return lax.dot_general(a, b, (((1,), (0,)), ((), ())), preferred_element_type=F32)


def dot_nt(a, b):
    return lax.dot_general(a, b, (((1,), (1,)), ((), ())), preferred_element_type=F32)


def whole(shape):
    return pl.BlockSpec(shape, lambda *_: (0,) * len(shape), pipeline_mode=pl.Buffered(1))


def sigmoid(g):
    return 0.5 * jnp.tanh(0.5 * g) + 0.5


def norm_rows(h):
    wide = h.astype(F32)
    scale = lax.rsqrt(jnp.mean(wide * wide, -1, keepdims=True) + EPS)
    return (wide * scale).astype(BF16)


def turn_step(j):
    return jnp.minimum(j, T // TURN - 1)


def pipelined(front, back):
    chunks = [pl.ds(i * CH, CH) for i in range(T // CH)]
    front(chunks[0])
    for i, rows in enumerate(chunks):
        if i + 1 < len(chunks):
            front(chunks[i + 1])
        back(rows)


def by_gate_and_up(g, u):
    s = sigmoid(g)
    sg = g * s
    return (sg * u).astype(BF16), u * (s + sg * (1.0 - s)), sg


def forward_kernel(x_ref, dy_ref, wg_ref, wu_ref, wd_ref, by_gate_ref, by_up_ref, hid_ref, h_ref, a_ref, at_ref, dyt_ref, a0, acc, g_s, u_s):
    j = pl.program_id(0)

    @pl.when(j == 0)
    def _():
        def prepare(i, _):
            rows = pl.ds(pl.multiple_of(i * CH, CH), CH)
            a0[rows, :] = norm_rows(x_ref[rows, :])
            acc[rows, :] = jnp.zeros((CH, D), F32)
            return 0

        lax.fori_loop(0, T // CH, prepare, 0)

    def front(rows):
        a = a0[rows, :]
        by_gate_ref[rows, :] = dot(a, wg_ref[0])
        by_up_ref[rows, :] = dot(a, wu_ref[0])

    def back(rows):
        g = by_gate_ref[rows, :]
        hid = (g * sigmoid(g) * by_up_ref[rows, :]).astype(BF16)
        hid_ref[rows, :] = hid
        acc[rows, :] += dot(hid, wd_ref[0])

    at_ref[...] = a0[pl.ds(pl.multiple_of(turn_step(j) * TURN, TURN), TURN), :].T
    dyt_ref[...] = dy_ref[...].T
    pipelined(front, back)

    @pl.when(j == NB - 1)
    def _():
        def finish(i, _):
            rows = pl.ds(pl.multiple_of(i * CH, CH), CH)
            h = (x_ref[rows, :].astype(F32) + acc[rows, :].astype(BF16).astype(F32)).astype(BF16)
            h_ref[rows, :] = h
            a_ref[rows, :] = norm_rows(h)
            return 0

        lax.fori_loop(0, T // CH, finish, 0)


def forward(x, dy, wg, wu, wd):
    return pl.pallas_call(
        forward_kernel,
        grid=(NB,),
        in_specs=[
            whole((T, D)),
            pl.BlockSpec((TURN, D), lambda j: (turn_step(j), 0)),
            pl.BlockSpec((1, D, BLK), lambda j: (0, 0, j)),
            pl.BlockSpec((1, D, BLK), lambda j: (0, 0, j)),
            pl.BlockSpec((1, BLK, D), lambda j: (0, j, 0)),
        ],
        out_specs=[
            pl.BlockSpec((T, BLK), lambda j: (0, j)),
            pl.BlockSpec((T, BLK), lambda j: (0, j)),
            pl.BlockSpec((T, BLK), lambda j: (0, j)),
            whole((T, D)),
            whole((T, D)),
            pl.BlockSpec((D, TURN), lambda j: (0, turn_step(j))),
            pl.BlockSpec((D, TURN), lambda j: (0, turn_step(j))),
        ],
        out_shape=[
            jax.ShapeDtypeStruct((T, FF), F32),
            jax.ShapeDtypeStruct((T, FF), F32),
            jax.ShapeDtypeStruct((T, FF), BF16),
            jax.ShapeDtypeStruct((T, D), BF16),
            jax.ShapeDtypeStruct((T, D), BF16),
            jax.ShapeDtypeStruct((D, T), BF16),
            jax.ShapeDtypeStruct((D, T), BF16),
        ],
        scratch_shapes=[pltpu.VMEM((T, D), BF16), pltpu.VMEM((T, D), F32), *[pltpu.VMEM((T, BLK), F32)] * 2],
        compiler_params=pltpu.CompilerParams(vmem_limit_bytes=VMEM_LIMIT),
        cost_estimate=pl.CostEstimate(flops=6 * T * D * FF, bytes_accessed=8 * T * FF, transcendentals=T * FF),
        name="fwd0",
    )(x, dy, wg, wu, wd)


SLOTS = 4
PAIR, FIRST, SECOND, BACK1, BACK2, BACK3 = 1, 2, 3, 4, 5, 6


def store_pieces(g_buf, slot, q, value):
    value = value.astype(BF16)
    for c in range(2):
        for ab in range(2):
            for s1 in range(2):
                for s2 in range(2):
                    x, y = (s1, s2) if ab == 0 else (s2, s1)
                    d = x * 4 + y * 2 + c
                    if q < 2:
                        r = d * 128 + ab * 64
                        g_buf[slot, c, ab, s1, s2, q] = value[r : r + 64]
                    else:
                        r = d * 32 + ab * 16
                        for k in range(4):
                            g_buf[slot, c, ab, s1, s2, q, k * 16 : k * 16 + 16] = value[r : r + 16, k * 256 : k * 256 + 256]


class Exchange:
    def __init__(self, scratch, f=None):
        self.g, self.h, self.q, self.e, self.r0, self.r1, self.r2 = scratch[:7]
        self.send, self.recv, self.keep, self.ahead = scratch[7:]
        self.f = f
        me = lax.axis_index("dp")
        self.rep = lax.axis_index("rep")
        self.x, self.y, self.c = me // 4, (me // 2) % 2, me % 2
        self.nx = (1 - self.x) * 4 + self.y * 2 + self.c
        self.ny = self.x * 4 + (1 - self.y) * 2 + self.c
        self.nc = self.x * 4 + self.y * 2 + (1 - self.c)

    def copy(self, kind, block, src, dst, to):
        slot = lax.rem(block, SLOTS)
        return pltpu.make_async_remote_copy(
            src_ref=src,
            dst_ref=dst,
            send_sem=self.send.at[kind, slot],
            recv_sem=self.recv.at[kind, slot],
            device_id=(self.rep, to),
            device_id_type=MESH,
        )

    def pair(self, b):
        return [self.copy(0, b, self.g.at[lax.rem(b, 2), 1 - self.c], self.r0.at[lax.rem(b, SLOTS)], self.nc)]

    def first(self, b):
        s, p = lax.rem(b, SLOTS), lax.rem(b, 2)
        return [
            self.copy(1, b, self.h.at[p, 0, 1 - self.x], self.r1.at[s, 0], self.nx),
            self.copy(2, b, self.h.at[p, 1, 1 - self.y], self.r1.at[s, 1], self.ny),
        ]

    def second(self, b):
        s, p = lax.rem(b, SLOTS), lax.rem(b, 2)
        return [
            self.copy(3, b, self.q.at[p, 0, 1 - self.y], self.r2.at[s, 0], self.ny),
            self.copy(4, b, self.q.at[p, 1, 1 - self.x], self.r2.at[s, 1], self.nx),
        ]

    def greet(self):
        barrier = pltpu.get_barrier_semaphore()
        for n in (self.nx, self.ny, self.nc):
            pl.semaphore_signal(barrier, inc=1, device_id=(self.rep, n), device_id_type=MESH)
        pl.semaphore_wait(barrier, 3)

    def wait_peers(self, count=1):
        for k in range(3):
            pl.semaphore_wait(self.ahead.at[k], count)

    def tell_peers(self):
        for k, n in enumerate((self.nx, self.ny, self.nc)):
            pl.semaphore_signal(self.ahead.at[k], inc=1, device_id=(self.rep, n), device_id_type=MESH)

    def mine(self, ab):
        return (self.x, self.y) if ab == 0 else (self.y, self.x)

    def own(self, b):
        return [pltpu.make_async_copy(self.e.at[lax.rem(b, SLOTS), ab], self.f.at[(b, self.c, ab, *self.mine(ab))], self.keep.at[lax.rem(b, SLOTS), ab]) for ab in range(2)]

    def back_first(self, b):
        return [self.copy(5 + ab, b, self.e.at[lax.rem(b, SLOTS), ab], self.f.at[(b, self.c, ab, *self.mine(ab))], (self.ny, self.nx)[ab]) for ab in range(2)]

    def back_second(self, b):
        out = []
        for ab in range(2):
            part = self.f.at[b, self.c, ab, self.mine(ab)[0]]
            out.append(self.copy(7 + ab, b, part, part, (self.nx, self.ny)[ab]))
        return out

    def back_pair(self, b):
        return [self.copy(9, b, self.f.at[b, self.c], self.f.at[b, self.c], self.nc)]

    def sums(self, b, out):
        s = lax.rem(b, SLOTS)
        for ab in range(2):
            s2 = self.mine(ab)[1]
            out[ab] = (self.q[lax.rem(b, 2), ab, s2].astype(F32) + self.r2[s, ab].astype(F32)).astype(BF16)

    def stages(self, t, gathered, e_refs):
        def at(lag, end, begin=0):
            return (t >= begin + lag) & (t < end + lag)

        @pl.when(at(PAIR, ALL))
        def _():
            b = t - PAIR
            s = lax.rem(b, SLOTS)
            g = lax.rem(b, 2)
            for cp in self.pair(b):
                cp.wait()

            def add(k, _):
                ab, s1, s2 = k // 4, (k // 2) % 2, k % 2
                self.h[g, ab, s1, s2] = (self.g[g, self.c, ab, s1, s2].astype(F32) + self.r0[s, ab, s1, s2].astype(F32)).astype(BF16)
                return 0

            lax.fori_loop(0, 8, add, 0)
            for cp in self.first(b):
                cp.start()

        @pl.when(at(FIRST, ALL))
        def _():
            b = t - FIRST
            s, p = lax.rem(b, SLOTS), lax.rem(b, 2)
            for cp in self.first(b):
                cp.wait()
            for ab in range(2):
                s1 = self.mine(ab)[0]
                for s2 in range(2):
                    self.q[p, ab, s2] = (self.h[p, ab, s1, s2].astype(F32) + self.r1[s, ab, s2].astype(F32)).astype(BF16)
            for cp in self.second(b):
                cp.start()

        @pl.when(at(SECOND, ALL))
        def _():
            for cp in self.second(t - SECOND):
                cp.wait()

        if gathered:

            @pl.when(at(SECOND, gathered))
            def _():
                b = t - SECOND
                self.sums(b, self.e.at[lax.rem(b, SLOTS)])
                for cp in self.own(b) + self.back_first(b):
                    cp.start()

        for begin, end, e_ref in e_refs:

            @pl.when(at(SECOND, end, begin))
            def _(e_ref=e_ref):
                self.sums(t - SECOND, e_ref.at[0])

        if gathered:

            @pl.when(at(BACK1, gathered))
            def _():
                for cp in self.own(t - BACK1) + self.back_first(t - BACK1):
                    cp.wait()
                for cp in self.back_second(t - BACK1):
                    cp.start()

            @pl.when(at(BACK2, gathered))
            def _():
                for cp in self.back_second(t - BACK2):
                    cp.wait()
                for cp in self.back_pair(t - BACK2):
                    cp.start()

            @pl.when(at(BACK3, gathered))
            def _():
                for cp in self.back_pair(t - BACK3):
                    cp.wait()


EXCHANGE_SCRATCH = [
    pltpu.VMEM((2, 2, 2, 2, 2, 3, 64, BLK), BF16),
    pltpu.VMEM((2, 2, 2, 2, 3, 64, BLK), BF16),
    pltpu.VMEM((2, 2, 2, 3, 64, BLK), BF16),
    pltpu.VMEM((SLOTS, 2, 3, 64, BLK), BF16),
    pltpu.VMEM((SLOTS, 2, 2, 2, 3, 64, BLK), BF16),
    pltpu.VMEM((SLOTS, 2, 2, 3, 64, BLK), BF16),
    pltpu.VMEM((SLOTS, 2, 3, 64, BLK), BF16),
    pltpu.SemaphoreType.DMA((10, SLOTS)),
    pltpu.SemaphoreType.DMA((10, SLOTS)),
    pltpu.SemaphoreType.DMA((SLOTS, 2)),
    pltpu.SemaphoreType.REGULAR((3,)),
]
ALL = 2 * NB
STEPS = ALL + SECOND
HALF = 7


def weight_grads(ex, t, at_ref, dt_ref, hid_s, dg_s, du_s):
    slot = lax.rem(t, 2)
    store_pieces(ex.g, slot, 0, dot(at_ref[...], dg_s[...]))
    store_pieces(ex.g, slot, 1, dot(at_ref[...], du_s[...]))
    store_pieces(ex.g, slot, 2, dot(dt_ref[...], hid_s[slot]).T)


def backward_kernel(
    a_hbm, dy_hbm, dyt_hbm, h_hbm, a0t_hbm, by_gate_hbm, by_up_hbm, hid_hbm, wg_ref, wu_ref, wd_ref,
    e0a_ref, e0b_ref, f_ref,
    a_s, at_s, d_s, dt_s, acc, g_s, u_s, dh_s, hid_s, dg_s, du_s, loads, *scratch,
):
    ex = Exchange(scratch, f_ref)
    t = pl.program_id(0)

    def load(k, src, dst):
        return pltpu.make_async_copy(src, dst, loads.at[k])

    def load_hidden(step):
        cols = pl.ds(pl.multiple_of((step - NB) * BLK, BLK), BLK)
        return [load(6, by_gate_hbm.at[:, cols], g_s), load(7, by_up_hbm.at[:, cols], u_s)]

    def load_units(step):
        cols = pl.ds(pl.multiple_of((step - NB) * BLK, BLK), BLK)
        return load(8 + lax.rem(step, 2), hid_hbm.at[:, cols], hid_s.at[lax.rem(step, 2)])

    load_a = load(0, a_hbm, a_s)
    other_loads = [load(1, dy_hbm, d_s), load(3, dyt_hbm, dt_s)]
    load_h = load(4, h_hbm, a_s)
    load_a0t = load(5, a0t_hbm, at_s)

    @pl.when(t == 0)
    def _():
        load_a.start()
        for cp in other_loads:
            cp.start()
        ex.greet()
        load_a.wait()

        def chunk(i, _):
            rows = pl.ds(pl.multiple_of(i * TURN, TURN), TURN)
            acc[rows, :] = jnp.zeros((TURN, D), F32)
            at_s[:, rows] = a_s[rows, :].T
            return 0

        lax.fori_loop(0, T // TURN, chunk, 0)
        for cp in other_loads:
            cp.wait()

    @pl.when(t >= 2)
    def _():
        ex.wait_peers()

    @pl.when((t >= NB - 1) & (t < ALL - 1))
    def _():
        load_units(t + 1).start()

    @pl.when(t < NB)
    def _():
        def front(rows):
            a = a_s[rows, :]
            g_s[rows, :] = dot(a, wg_ref[0])
            u_s[rows, :] = dot(a, wu_ref[0])
            dh_s[rows, :] = dot_nt(d_s[rows, :], wd_ref[0])

        def back(rows):
            hid_s[lax.rem(t, 2), rows, :], by_gate, by_up = by_gate_and_up(g_s[rows, :], u_s[rows, :])
            dh = dh_s[rows, :].astype(BF16).astype(F32)
            dgate = (dh * by_gate).astype(BF16)
            dup = (dh * by_up).astype(BF16)
            dg_s[rows, :] = dgate
            du_s[rows, :] = dup
            acc[rows, :] += dot_nt(dgate, wg_ref[0]) + dot_nt(dup, wu_ref[0])

        pipelined(front, back)
        weight_grads(ex, t, at_s, dt_s, hid_s, dg_s, du_s)

    @pl.when(t == NB - 1)
    def _():
        load_h.start()
        load_a0t.start()
        for cp in load_hidden(t + 1):
            cp.start()

    @pl.when(t == NB)
    def _():
        load_h.wait()

        def chunk(i, _):
            rows = pl.ds(pl.multiple_of(i * 256, 256), 256)
            wide = a_s[rows, :].astype(F32)
            da = acc[rows, :].astype(BF16).astype(F32)
            scale = lax.rsqrt(jnp.mean(wide * wide, -1, keepdims=True) + EPS)
            inner = jnp.mean(da * wide, -1, keepdims=True)
            back = (da * scale - wide * (scale * scale * scale * inner)).astype(BF16)
            dh = (d_s[rows, :].astype(F32) + back.astype(F32)).astype(BF16)
            d_s[rows, :] = dh
            dt_s[:, rows] = dh.T
            return 0

        lax.fori_loop(0, T // 256, chunk, 0)
        load_a0t.wait()

    @pl.when((t >= NB) & (t < ALL))
    def _():
        for cp in [*load_hidden(t), load_units(t)]:
            cp.wait()

        def front(rows):
            dh_s[rows, :] = dot_nt(d_s[rows, :], wd_ref[0])

        def back(rows):
            dh = dh_s[rows, :].astype(BF16).astype(F32)
            _, by_gate, by_up = by_gate_and_up(g_s[rows, :], u_s[rows, :])
            dg_s[rows, :] = (dh * by_gate).astype(BF16)
            du_s[rows, :] = (dh * by_up).astype(BF16)

        pipelined(front, back)

        @pl.when(t < ALL - 1)
        def _():
            for cp in load_hidden(t + 1):
                cp.start()

        weight_grads(ex, t, at_s, dt_s, hid_s, dg_s, du_s)

    @pl.when(t < ALL)
    def _():
        for cp in ex.pair(t):
            cp.start()

    ex.stages(t, NB, [(NB, NB + HALF, e0a_ref), (NB + HALF, ALL, e0b_ref)])
    ex.tell_peers()

    @pl.when(t == STEPS - 1)
    def _():
        ex.wait_peers(2)


PIECES = (2, 3, 64, BLK)
FULL = (2, 2, 2, 2, 3, 64, BLK)


def sums_spec(begin, end):
    return pl.BlockSpec((1,) + PIECES, lambda t: (jnp.clip(t - SECOND - begin, 0, end - begin - 1), 0, 0, 0, 0))


def sums_shape(begin, end):
    return jax.ShapeDtypeStruct((end - begin,) + PIECES, BF16)


def backward(a, dy, dyt, h, a0t, by_gate, by_up, hid, wg, wu, wd):
    any_spec = pl.BlockSpec(memory_space=pl.ANY)
    wide = pl.BlockSpec((1, D, BLK), lambda t: (1, 0, jnp.minimum(t, NB - 1)))
    tall = pl.BlockSpec((1, BLK, D), lambda t: (jnp.where(t < NB, 1, 0), jnp.where(t < NB, t, jnp.minimum(t, ALL - 1) - NB), 0))
    ends = [(NB, NB + HALF), (NB + HALF, ALL)]
    return pl.pallas_call(
        backward_kernel,
        grid=(STEPS,),
        in_specs=[any_spec] * 8 + [wide, wide, tall],
        out_specs=[*[sums_spec(*e) for e in ends], any_spec],
        out_shape=[*[sums_shape(*e) for e in ends], jax.ShapeDtypeStruct((NB,) + FULL, BF16)],
        scratch_shapes=[
            pltpu.VMEM((T, D), BF16),
            pltpu.VMEM((D, T), BF16),
            pltpu.VMEM((T, D), BF16),
            pltpu.VMEM((D, T), BF16),
            pltpu.VMEM((T, D), F32),
            *[pltpu.VMEM((T, BLK), F32)] * 3,
            pltpu.VMEM((2, T, BLK), BF16),
            *[pltpu.VMEM((T, BLK), BF16)] * 2,
            pltpu.SemaphoreType.DMA((10,)),
            *EXCHANGE_SCRATCH,
        ],
        compiler_params=pltpu.CompilerParams(vmem_limit_bytes=VMEM_LIMIT, collective_id=0, has_side_effects=True),
        cost_estimate=pl.CostEstimate(flops=24 * T * D * FF, bytes_accessed=12 * T * FF, transcendentals=2 * T * FF),
        name="backward",
    )(a, dy, dyt, h, a0t, by_gate, by_up, hid, wg, wu, wd)


def adamw(w, m, v, g):
    m = 0.9 * m + 0.1 * g
    v = 0.95 * v + 0.05 * g * g
    step = m * lax.rsqrt(v + 1e-8) + 0.1 * w
    return (w - 0.02 * step).astype(BF16), m, v


def adamw_kernel(own, g_ref, *refs):
    ins, outs = refs[:9], refs[-9:]
    for x, y, c, ab in itertools.product(range(2), repeat=4):
        d = x * 4 + y * 2 + c
        at = (d, 0, ab) if not own else (0, c, ab, x, y) if ab == 0 else (0, c, ab, y, x)
        for q in range(3):
            w_ref, m_ref, v_ref = ins[q], ins[3 + q], ins[6 + q]
            wo_ref, mo_ref, vo_ref = outs[q], outs[3 + q], outs[6 + q]
            if q < 2:
                parts = [(pl.ds(d * 128 + ab * 64, 64), slice(None), slice(None))]
            else:
                parts = [(pl.ds(d * 32 + ab * 16, 16), pl.ds(k * 256, 256), pl.ds(k * 16, 16)) for k in range(4)]
            for r, cols, of in parts:
                g = g_ref[(*at, q, of)].astype(F32)
                wo_ref[0, r, cols], mo_ref[0, r, cols], vo_ref[0, r, cols] = adamw(
                    w_ref[0, r, cols].astype(F32), m_ref[0, r, cols], v_ref[0, r, cols], g
                )


def update(layer, begin, g, arrays, before):
    own = g.ndim == 8
    count = g.shape[0] if own else g.shape[1]
    g_spec = pl.BlockSpec((1,) + FULL, lambda j: (j,) + (0,) * 7) if own else pl.BlockSpec((8, 1) + PIECES, lambda j: (0, j, 0, 0, 0, 0))
    wide = pl.BlockSpec((1, D, BLK), lambda j: (layer, 0, begin + j))
    tall = pl.BlockSpec((1, BLK, D), lambda j: (layer, begin + j, 0))
    specs = [wide, wide, tall] * 3
    held = [] if before is None else list(before)
    size = 3 * D * BLK * count
    return pl.pallas_call(
        functools.partial(adamw_kernel, own),
        grid=(count,),
        in_specs=[g_spec, *specs, *[pl.BlockSpec(memory_space=pl.ANY)] * len(held)],
        out_specs=specs,
        out_shape=[jax.ShapeDtypeStruct(a.shape, a.dtype) for a in arrays],
        input_output_aliases={10 + i: i for i in range(len(held))},
        compiler_params=pltpu.CompilerParams(vmem_limit_bytes=VMEM_LIMIT),
        cost_estimate=pl.CostEstimate(flops=30 * size, bytes_accessed=22 * size, transcendentals=size),
        name=f"adamw{layer}_{begin}",
    )(g, *arrays, *held)


def solution(mesh):
    def step(x, dy, wg, wu, wd, *moments):
        x, dy = x[0], dy[0]
        by_gate, by_up, hid, h1, a1, a0t, dyt = forward(x, dy, wg, wu, wd)
        e0a, e0b, f1 = backward(a1, dy, dyt, h1, a0t, by_gate, by_up, hid, wg, wu, wd)
        g0a, g0b = (lax.all_gather(e, "dp", axis=0, tiled=False) for e in (e0a, e0b))
        arrays = (wg, wu, wd, *moments)
        new = update(1, 0, f1, arrays, None)
        new = update(0, 0, g0a, arrays, new)
        return tuple(update(0, HALF, g0b, arrays, new))

    return jax.shard_map(
        step,
        mesh=mesh,
        in_specs=(P(("rep", "dp"), None, None),) * 2 + (P(None, None, None),) * 9,
        out_specs=(P("rep", None, None),) * 9,
        check_vma=False,
    )
```

```python
import functools
import itertools

import jax
import jax.numpy as jnp
from jax import lax
from jax.experimental import pallas as pl
from jax.experimental.pallas import tpu as pltpu
from jax.sharding import PartitionSpec as P

F32, BF16 = jnp.float32, jnp.bfloat16
T, D, FF = 2048, 1024, 3328
BLK = 256
NB = FF // BLK
CH = 512
TURN = 256
EPS = 1e-6
MESH = pl.DeviceIdType.MESH
VMEM_LIMIT = 64 * 1024 * 1024 - 65536 - 1024 * 1024


def dot(a, b):
    return lax.dot_general(a, b, (((1,), (0,)), ((), ())), preferred_element_type=F32)


def dot_nt(a, b):
    return lax.dot_general(a, b, (((1,), (1,)), ((), ())), preferred_element_type=F32)


def whole(shape):
    return pl.BlockSpec(shape, lambda *_: (0,) * len(shape), pipeline_mode=pl.Buffered(1))


def sigmoid(g):
    return 0.5 * jnp.tanh(0.5 * g) + 0.5


def norm_rows(h):
    wide = h.astype(F32)
    scale = lax.rsqrt(jnp.mean(wide * wide, -1, keepdims=True) + EPS)
    return (wide * scale).astype(BF16)


def turn_step(j):
    return jnp.minimum(j, T // TURN - 1)


def pipelined(front, back):
    chunks = [pl.ds(i * CH, CH) for i in range(T // CH)]
    front(chunks[0])
    for i, rows in enumerate(chunks):
        if i + 1 < len(chunks):
            front(chunks[i + 1])
        back(rows)


def by_gate_and_up(g, u):
    s = sigmoid(g)
    sg = g * s
    return (sg * u).astype(BF16), u * (s + sg * (1.0 - s)), sg


def forward_kernel(x_ref, dy_ref, wg_ref, wu_ref, wd_ref, gate_ref, up_ref, h_ref, a_ref, at_ref, dyt_ref, a0, acc, g_s, u_s):
    j = pl.program_id(0)

    @pl.when(j == 0)
    def _():
        def prepare(i, _):
            rows = pl.ds(pl.multiple_of(i * CH, CH), CH)
            a0[rows, :] = norm_rows(x_ref[rows, :])
            acc[rows, :] = jnp.zeros((CH, D), F32)
            return 0

        lax.fori_loop(0, T // CH, prepare, 0)

    def front(rows):
        a = a0[rows, :]
        gate_ref[rows, :] = dot(a, wg_ref[0])
        up_ref[rows, :] = dot(a, wu_ref[0])

    def back(rows):
        g = gate_ref[rows, :]
        hid = (g * sigmoid(g) * up_ref[rows, :]).astype(BF16)
        acc[rows, :] += dot(hid, wd_ref[0])

    at_ref[...] = a0[pl.ds(pl.multiple_of(turn_step(j) * TURN, TURN), TURN), :].T
    dyt_ref[...] = dy_ref[...].T
    pipelined(front, back)

    @pl.when(j == NB - 1)
    def _():
        def finish(i, _):
            rows = pl.ds(pl.multiple_of(i * CH, CH), CH)
            h = (x_ref[rows, :].astype(F32) + acc[rows, :].astype(BF16).astype(F32)).astype(BF16)
            h_ref[rows, :] = h
            a_ref[rows, :] = norm_rows(h)
            return 0

        lax.fori_loop(0, T // CH, finish, 0)


def forward(x, dy, wg, wu, wd):
    return pl.pallas_call(
        forward_kernel,
        grid=(NB,),
        in_specs=[
            whole((T, D)),
            pl.BlockSpec((TURN, D), lambda j: (turn_step(j), 0)),
            pl.BlockSpec((1, D, BLK), lambda j: (0, 0, j)),
            pl.BlockSpec((1, D, BLK), lambda j: (0, 0, j)),
            pl.BlockSpec((1, BLK, D), lambda j: (0, j, 0)),
        ],
        out_specs=[
            pl.BlockSpec((T, BLK), lambda j: (0, j)),
            pl.BlockSpec((T, BLK), lambda j: (0, j)),
            whole((T, D)),
            whole((T, D)),
            pl.BlockSpec((D, TURN), lambda j: (0, turn_step(j))),
            pl.BlockSpec((D, TURN), lambda j: (0, turn_step(j))),
        ],
        out_shape=[
            jax.ShapeDtypeStruct((T, FF), F32),
            jax.ShapeDtypeStruct((T, FF), F32),
            jax.ShapeDtypeStruct((T, D), BF16),
            jax.ShapeDtypeStruct((T, D), BF16),
            jax.ShapeDtypeStruct((D, T), BF16),
            jax.ShapeDtypeStruct((D, T), BF16),
        ],
        scratch_shapes=[pltpu.VMEM((T, D), BF16), pltpu.VMEM((T, D), F32), *[pltpu.VMEM((T, BLK), F32)] * 2],
        compiler_params=pltpu.CompilerParams(vmem_limit_bytes=VMEM_LIMIT),
        cost_estimate=pl.CostEstimate(flops=6 * T * D * FF, bytes_accessed=8 * T * FF, transcendentals=T * FF),
        name="fwd0",
    )(x, dy, wg, wu, wd)


SLOTS = 4
PAIR, FIRST, SECOND, BACK1, BACK2, BACK3 = 1, 2, 3, 4, 5, 6
FIRST_LATE, SECOND_LATE = 3, 5


def store_pieces(g_buf, slot, q, value):
    value = value.astype(BF16)
    for c in range(2):
        for ab in range(2):
            for s1 in range(2):
                for s2 in range(2):
                    x, y = (s1, s2) if ab == 0 else (s2, s1)
                    d = x * 4 + y * 2 + c
                    if q < 2:
                        r = d * 128 + ab * 64
                        g_buf[slot, c, ab, s1, s2, q] = value[r : r + 64]
                    else:
                        r = d * 32 + ab * 16
                        for k in range(4):
                            g_buf[slot, c, ab, s1, s2, q, k * 16 : k * 16 + 16] = value[r : r + 16, k * 256 : k * 256 + 256]


class Exchange:
    def __init__(self, scratch, f=None):
        self.g, self.h, self.q, self.e, self.r0, self.r1, self.r2 = scratch[:7]
        self.send, self.recv, self.keep, self.ahead = scratch[7:]
        self.f = f
        me = lax.axis_index("dp")
        self.rep = lax.axis_index("rep")
        self.x, self.y, self.c = me // 4, (me // 2) % 2, me % 2
        self.nx = (1 - self.x) * 4 + self.y * 2 + self.c
        self.ny = self.x * 4 + (1 - self.y) * 2 + self.c
        self.nc = self.x * 4 + self.y * 2 + (1 - self.c)

    def copy(self, kind, block, src, dst, to):
        slot = lax.rem(block, SLOTS)
        return pltpu.make_async_remote_copy(
            src_ref=src,
            dst_ref=dst,
            send_sem=self.send.at[kind, slot],
            recv_sem=self.recv.at[kind, slot],
            device_id=(self.rep, to),
            device_id_type=MESH,
        )

    def pair(self, b):
        return [self.copy(0, b, self.g.at[lax.rem(b, 2), 1 - self.c], self.r0.at[lax.rem(b, SLOTS)], self.nc)]

    def first(self, b):
        s = lax.rem(b, SLOTS)
        return [
            self.copy(1, b, self.h.at[s, 0, 1 - self.x], self.r1.at[s, 0], self.nx),
            self.copy(2, b, self.h.at[s, 1, 1 - self.y], self.r1.at[s, 1], self.ny),
        ]

    def second(self, b):
        s = lax.rem(b, SLOTS)
        return [
            self.copy(3, b, self.q.at[s, 0, 1 - self.y], self.r2.at[s, 0], self.ny),
            self.copy(4, b, self.q.at[s, 1, 1 - self.x], self.r2.at[s, 1], self.nx),
        ]

    def greet(self):
        barrier = pltpu.get_barrier_semaphore()
        for n in (self.nx, self.ny, self.nc):
            pl.semaphore_signal(barrier, inc=1, device_id=(self.rep, n), device_id_type=MESH)
        pl.semaphore_wait(barrier, 3)

    def wait_peers(self, count=1):
        for k in range(3):
            pl.semaphore_wait(self.ahead.at[k], count)

    def tell_peers(self):
        for k, n in enumerate((self.nx, self.ny, self.nc)):
            pl.semaphore_signal(self.ahead.at[k], inc=1, device_id=(self.rep, n), device_id_type=MESH)

    def mine(self, ab):
        return (self.x, self.y) if ab == 0 else (self.y, self.x)

    def own(self, b):
        return [pltpu.make_async_copy(self.e.at[lax.rem(b, SLOTS), ab], self.f.at[(b, self.c, ab, *self.mine(ab))], self.keep.at[lax.rem(b, SLOTS), ab]) for ab in range(2)]

    def back_first(self, b):
        return [self.copy(5 + ab, b, self.e.at[lax.rem(b, SLOTS), ab], self.f.at[(b, self.c, ab, *self.mine(ab))], (self.ny, self.nx)[ab]) for ab in range(2)]

    def back_second(self, b):
        out = []
        for ab in range(2):
            part = self.f.at[b, self.c, ab, self.mine(ab)[0]]
            out.append(self.copy(7 + ab, b, part, part, (self.nx, self.ny)[ab]))
        return out

    def back_pair(self, b):
        return [self.copy(9, b, self.f.at[b, self.c], self.f.at[b, self.c], self.nc)]

    def sums(self, b, out):
        s = lax.rem(b, SLOTS)
        for ab in range(2):
            s2 = self.mine(ab)[1]
            out[ab] = (self.q[s, ab, s2].astype(F32) + self.r2[s, ab].astype(F32)).astype(BF16)

    def stages(self, t, gathered, e_refs):
        def at(lag, end, begin=0):
            return (t >= begin + lag) & (t < end + lag)

        @pl.when(at(PAIR, ALL))
        def _():
            b = t - PAIR
            s = lax.rem(b, SLOTS)
            g = lax.rem(b, 2)
            for cp in self.pair(b):
                cp.wait()

            def add(k, _):
                ab, s1, s2 = k // 4, (k // 2) % 2, k % 2
                self.h[s, ab, s1, s2] = (self.g[g, self.c, ab, s1, s2].astype(F32) + self.r0[s, ab, s1, s2].astype(F32)).astype(BF16)
                return 0

            lax.fori_loop(0, 8, add, 0)
            for cp in self.first(b):
                cp.start()

        def first_stage(b):
            s = lax.rem(b, SLOTS)
            for cp in self.first(b):
                cp.wait()
            for ab in range(2):
                s1 = self.mine(ab)[0]
                for s2 in range(2):
                    self.q[s, ab, s2] = (self.h[s, ab, s1, s2].astype(F32) + self.r1[s, ab, s2].astype(F32)).astype(BF16)
            for cp in self.second(b):
                cp.start()

        @pl.when(at(FIRST, gathered))
        def _():
            first_stage(t - FIRST)

        @pl.when(at(FIRST_LATE, ALL, gathered))
        def _():
            first_stage(t - FIRST_LATE)

        @pl.when(at(SECOND, gathered))
        def _():
            b = t - SECOND
            for cp in self.second(b):
                cp.wait()
            self.sums(b, self.e.at[lax.rem(b, SLOTS)])
            for cp in self.own(b) + self.back_first(b):
                cp.start()

        for begin, end, e_ref in e_refs:

            @pl.when(at(SECOND_LATE, end, begin))
            def _(e_ref=e_ref):
                b = t - SECOND_LATE
                for cp in self.second(b):
                    cp.wait()
                self.sums(b, e_ref.at[0])

        if gathered:

            @pl.when(at(BACK1, gathered))
            def _():
                for cp in self.own(t - BACK1) + self.back_first(t - BACK1):
                    cp.wait()
                for cp in self.back_second(t - BACK1):
                    cp.start()

            @pl.when(at(BACK2, gathered))
            def _():
                for cp in self.back_second(t - BACK2):
                    cp.wait()
                for cp in self.back_pair(t - BACK2):
                    cp.start()

            @pl.when(at(BACK3, gathered))
            def _():
                for cp in self.back_pair(t - BACK3):
                    cp.wait()


EXCHANGE_SCRATCH = [
    pltpu.VMEM((2, 2, 2, 2, 2, 3, 64, BLK), BF16),
    pltpu.VMEM((SLOTS, 2, 2, 2, 3, 64, BLK), BF16),
    pltpu.VMEM((SLOTS, 2, 2, 3, 64, BLK), BF16),
    pltpu.VMEM((SLOTS, 2, 3, 64, BLK), BF16),
    pltpu.VMEM((SLOTS, 2, 2, 2, 3, 64, BLK), BF16),
    pltpu.VMEM((SLOTS, 2, 2, 3, 64, BLK), BF16),
    pltpu.VMEM((SLOTS, 2, 3, 64, BLK), BF16),
    pltpu.SemaphoreType.DMA((10, SLOTS)),
    pltpu.SemaphoreType.DMA((10, SLOTS)),
    pltpu.SemaphoreType.DMA((SLOTS, 2)),
    pltpu.SemaphoreType.REGULAR((3,)),
]
ALL = 2 * NB
STEPS = ALL + SECOND_LATE
HALF = 7


def weight_grads(ex, t, at_ref, dt_ref, hid_s, dg_s, du_s):
    slot = lax.rem(t, 2)
    store_pieces(ex.g, slot, 0, dot(at_ref[...], dg_s[...]))
    store_pieces(ex.g, slot, 1, dot(at_ref[...], du_s[...]))
    store_pieces(ex.g, slot, 2, dot(dt_ref[...], hid_s[...]).T)


def backward_kernel(
    a_hbm, dy_hbm, dyt_hbm, h_hbm, a0t_hbm, gate_hbm, up_hbm, wg_ref, wu_ref, wd_ref,
    e0a_ref, e0b_ref, f_ref,
    a_s, at_s, d_s, dt_s, acc, g_s, u_s, dh_s, hid_s, dg_s, du_s, loads, *scratch,
):
    ex = Exchange(scratch, f_ref)
    t = pl.program_id(0)

    def load(k, src, dst):
        return pltpu.make_async_copy(src, dst, loads.at[k])

    def load_hidden(step):
        cols = pl.ds(pl.multiple_of((step - NB) * BLK, BLK), BLK)
        return [load(6, gate_hbm.at[:, cols], g_s), load(7, up_hbm.at[:, cols], u_s)]

    load_a = load(0, a_hbm, a_s)
    other_loads = [load(1, dy_hbm, d_s), load(3, dyt_hbm, dt_s)]
    load_h = load(4, h_hbm, a_s)
    load_a0t = load(5, a0t_hbm, at_s)

    @pl.when(t == 0)
    def _():
        load_a.start()
        for cp in other_loads:
            cp.start()
        ex.greet()
        load_a.wait()

        def chunk(i, _):
            rows = pl.ds(pl.multiple_of(i * TURN, TURN), TURN)
            acc[rows, :] = jnp.zeros((TURN, D), F32)
            at_s[:, rows] = a_s[rows, :].T
            return 0

        lax.fori_loop(0, T // TURN, chunk, 0)
        for cp in other_loads:
            cp.wait()

    @pl.when(t >= 2)
    def _():
        ex.wait_peers()

    @pl.when(t < NB)
    def _():
        def front(rows):
            a = a_s[rows, :]
            g_s[rows, :] = dot(a, wg_ref[0])
            u_s[rows, :] = dot(a, wu_ref[0])
            dh_s[rows, :] = dot_nt(d_s[rows, :], wd_ref[0])

        def back(rows):
            hid_s[rows, :], by_gate, by_up = by_gate_and_up(g_s[rows, :], u_s[rows, :])
            dh = dh_s[rows, :].astype(BF16).astype(F32)
            dgate = (dh * by_gate).astype(BF16)
            dup = (dh * by_up).astype(BF16)
            dg_s[rows, :] = dgate
            du_s[rows, :] = dup
            acc[rows, :] += dot_nt(dgate, wg_ref[0]) + dot_nt(dup, wu_ref[0])

        pipelined(front, back)
        weight_grads(ex, t, at_s, dt_s, hid_s, dg_s, du_s)

    @pl.when(t == NB - 1)
    def _():
        load_h.start()
        load_a0t.start()
        for cp in load_hidden(t + 1):
            cp.start()

    @pl.when(t == NB)
    def _():
        load_h.wait()

        def chunk(i, _):
            rows = pl.ds(pl.multiple_of(i * 256, 256), 256)
            wide = a_s[rows, :].astype(F32)
            da = acc[rows, :].astype(BF16).astype(F32)
            scale = lax.rsqrt(jnp.mean(wide * wide, -1, keepdims=True) + EPS)
            inner = jnp.mean(da * wide, -1, keepdims=True)
            back = (da * scale - wide * (scale * scale * scale * inner)).astype(BF16)
            dh = (d_s[rows, :].astype(F32) + back.astype(F32)).astype(BF16)
            d_s[rows, :] = dh
            dt_s[:, rows] = dh.T
            return 0

        lax.fori_loop(0, T // 256, chunk, 0)
        load_a0t.wait()

    @pl.when((t >= NB) & (t < ALL))
    def _():
        for cp in load_hidden(t):
            cp.wait()

        def front(rows):
            dh_s[rows, :] = dot_nt(d_s[rows, :], wd_ref[0])

        def back(rows):
            dh = dh_s[rows, :].astype(BF16).astype(F32)
            hid_s[rows, :], by_gate, by_up = by_gate_and_up(g_s[rows, :], u_s[rows, :])
            dg_s[rows, :] = (dh * by_gate).astype(BF16)
            du_s[rows, :] = (dh * by_up).astype(BF16)

        pipelined(front, back)

        @pl.when(t < ALL - 1)
        def _():
            for cp in load_hidden(t + 1):
                cp.start()

        weight_grads(ex, t, at_s, dt_s, hid_s, dg_s, du_s)

    @pl.when(t < ALL)
    def _():
        for cp in ex.pair(t):
            cp.start()

    ex.stages(t, NB, [(NB, NB + HALF, e0a_ref), (NB + HALF, ALL, e0b_ref)])
    ex.tell_peers()

    @pl.when(t == STEPS - 1)
    def _():
        ex.wait_peers(2)


PIECES = (2, 3, 64, BLK)
FULL = (2, 2, 2, 2, 3, 64, BLK)


def sums_spec(begin, end):
    return pl.BlockSpec((1,) + PIECES, lambda t: (jnp.clip(t - SECOND_LATE - begin, 0, end - begin - 1), 0, 0, 0, 0))


def sums_shape(begin, end):
    return jax.ShapeDtypeStruct((end - begin,) + PIECES, BF16)


def backward(a, dy, dyt, h, a0t, gate, up, wg, wu, wd):
    any_spec = pl.BlockSpec(memory_space=pl.ANY)
    wide = pl.BlockSpec((1, D, BLK), lambda t: (1, 0, jnp.minimum(t, NB - 1)))
    tall = pl.BlockSpec((1, BLK, D), lambda t: (jnp.where(t < NB, 1, 0), jnp.where(t < NB, t, jnp.minimum(t, ALL - 1) - NB), 0))
    ends = [(NB, NB + HALF), (NB + HALF, ALL)]
    return pl.pallas_call(
        backward_kernel,
        grid=(STEPS,),
        in_specs=[any_spec] * 7 + [wide, wide, tall],
        out_specs=[*[sums_spec(*e) for e in ends], any_spec],
        out_shape=[*[sums_shape(*e) for e in ends], jax.ShapeDtypeStruct((NB,) + FULL, BF16)],
        scratch_shapes=[
            pltpu.VMEM((T, D), BF16),
            pltpu.VMEM((D, T), BF16),
            pltpu.VMEM((T, D), BF16),
            pltpu.VMEM((D, T), BF16),
            pltpu.VMEM((T, D), F32),
            *[pltpu.VMEM((T, BLK), F32)] * 3,
            *[pltpu.VMEM((T, BLK), BF16)] * 3,
            pltpu.SemaphoreType.DMA((8,)),
            *EXCHANGE_SCRATCH,
        ],
        compiler_params=pltpu.CompilerParams(vmem_limit_bytes=VMEM_LIMIT, collective_id=0, has_side_effects=True),
        cost_estimate=pl.CostEstimate(flops=24 * T * D * FF, bytes_accessed=12 * T * FF, transcendentals=2 * T * FF),
        name="backward",
    )(a, dy, dyt, h, a0t, gate, up, wg, wu, wd)


def adamw(w, m, v, g):
    m = 0.9 * m + 0.1 * g
    v = 0.95 * v + 0.05 * g * g
    step = m * lax.rsqrt(v + 1e-8) + 0.1 * w
    return (w - 0.02 * step).astype(BF16), m, v


def adamw_kernel(own, g_ref, *refs):
    ins, outs = refs[:9], refs[-9:]
    for x, y, c, ab in itertools.product(range(2), repeat=4):
        d = x * 4 + y * 2 + c
        at = (d, 0, ab) if not own else (0, c, ab, x, y) if ab == 0 else (0, c, ab, y, x)
        for q in range(3):
            w_ref, m_ref, v_ref = ins[q], ins[3 + q], ins[6 + q]
            wo_ref, mo_ref, vo_ref = outs[q], outs[3 + q], outs[6 + q]
            if q < 2:
                parts = [(pl.ds(d * 128 + ab * 64, 64), slice(None), slice(None))]
            else:
                parts = [(pl.ds(d * 32 + ab * 16, 16), pl.ds(k * 256, 256), pl.ds(k * 16, 16)) for k in range(4)]
            for r, cols, of in parts:
                g = g_ref[(*at, q, of)].astype(F32)
                wo_ref[0, r, cols], mo_ref[0, r, cols], vo_ref[0, r, cols] = adamw(
                    w_ref[0, r, cols].astype(F32), m_ref[0, r, cols], v_ref[0, r, cols], g
                )


def update(layer, begin, g, arrays, before):
    own = g.ndim == 8
    count = g.shape[0] if own else g.shape[1]
    g_spec = pl.BlockSpec((1,) + FULL, lambda j: (j,) + (0,) * 7) if own else pl.BlockSpec((8, 1) + PIECES, lambda j: (0, j, 0, 0, 0, 0))
    wide = pl.BlockSpec((1, D, BLK), lambda j: (layer, 0, begin + j))
    tall = pl.BlockSpec((1, BLK, D), lambda j: (layer, begin + j, 0))
    specs = [wide, wide, tall] * 3
    held = [] if before is None else list(before)
    size = 3 * D * BLK * count
    return pl.pallas_call(
        functools.partial(adamw_kernel, own),
        grid=(count,),
        in_specs=[g_spec, *specs, *[pl.BlockSpec(memory_space=pl.ANY)] * len(held)],
        out_specs=specs,
        out_shape=[jax.ShapeDtypeStruct(a.shape, a.dtype) for a in arrays],
        input_output_aliases={10 + i: i for i in range(len(held))},
        compiler_params=pltpu.CompilerParams(vmem_limit_bytes=VMEM_LIMIT),
        cost_estimate=pl.CostEstimate(flops=30 * size, bytes_accessed=22 * size, transcendentals=size),
        name=f"adamw{layer}_{begin}",
    )(g, *arrays, *held)


def solution(mesh):
    def step(x, dy, wg, wu, wd, *moments):
        x, dy = x[0], dy[0]
        gate, up, h1, a1, a0t, dyt = forward(x, dy, wg, wu, wd)
        e0a, e0b, f1 = backward(a1, dy, dyt, h1, a0t, gate, up, wg, wu, wd)
        g0a, g0b = (lax.all_gather(e, "dp", axis=0, tiled=False) for e in (e0a, e0b))
        arrays = (wg, wu, wd, *moments)
        new = update(1, 0, f1, arrays, None)
        new = update(0, 0, g0a, arrays, new)
        return tuple(update(0, HALF, g0b, arrays, new))

    return jax.shard_map(
        step,
        mesh=mesh,
        in_specs=(P(("rep", "dp"), None, None),) * 2 + (P(None, None, None),) * 9,
        out_specs=(P("rep", None, None),) * 9,
        check_vma=False,
    )
```
